512 devices in a mesh: mem: 32 (over z_hi, x, core), lat: 16 (over y, z_lo).
Axes of the slice: x: 4, y: 4, z: 16 (z_hi: 4, z_lo: 4; z = z_hi * 4 + z_lo), core: 2. Of those that a mesh axis runs over, the one named last changes fastest.
Arguments:
- fields: float32 [1024, 128, 256], P('mem', 'lat'), may hold values from -8 to 8
- forcing: float32 [128, 256], P('lat'), may hold values from 2 to 8
- obs_cell: int32 [16, 32, 256], P('lat'), may hold values from 0 to 63
- obs_count: int32 [16, 32], P('lat', 'mem'), may hold values from 64 to 256, as said below
- obs_value: float32 [16, 32, 256], P('lat', 'mem'), may hold values from -12 to 12
- obs_var: float32 [16, 32, 256], P('lat', 'mem'), may hold values from 0.25 to 1
Outputs:
- analysis: float32 [1024, 128, 256], P('mem', 'lat')
The draws below stay inside these ranges and needn't reach their ends.
Inputs may be any that keep to these rules, and one draw needn't show every extreme that they name: `obs_count`: each latitude strip has a patch with exactly 256 live observations.
All inputs are finite; a program needn't handle non-finite values.
Results may differ from the reference program's by a relative error of at most 0.0003.
Values sent between devices are 32-bit elements; how exact they have to be, the bound alone decides.
No kernel may reach another device: no remote copies, remote signals or barrier semaphores. Data moves between devices by JAX's collectives and lax.ppermute only.
A program may use at most 64 MiB of HBM per device.

```python
import math
import jax
import jax.numpy as jnp
from jax import lax

MEMBERS = 1024
OBS = 256
PATCH_CELLS = 64
NLON = 256
STEPS = 4
NROWS = 128
PATCHES_STRIP = 32
N_LAT = 16


def draw_obs_count(key, part):
    first_key = jax.random.fold_in(key, 11)
    second_key = jax.random.fold_in(key, 23)
    drawn = jax.random.randint(first_key, (N_LAT, PATCHES_STRIP), OBS // 4, OBS + 1)
    chosen_slot = jax.random.randint(second_key, (N_LAT, 1), 0, PATCHES_STRIP)
    picked = jnp.arange(PATCHES_STRIP)[None, :] == chosen_slot
    return jnp.where(picked, OBS, drawn).astype(jnp.int32)


def touch_ends(values, key, smallest, top_value):
    index_at = [jax.random.randint(jax.random.fold_in(key, axis), (), 0, length) for axis, length in enumerate(values.shape)]
    widest = values.shape.index(max(values.shape))
    beside = index_at[:widest] + [(index_at[widest] + 1) % values.shape[widest]] + index_at[widest + 1:]
    return values.at[tuple(index_at)].set(smallest).at[tuple(beside)].set(top_value)


def block_scale(own_key, dims, cuts, smallest, largest):
    gain, own = 1.0, jax.random.fold_in(own_key, 6)
    for position, parts in cuts:
        draws = jnp.exp(jax.random.uniform(jax.random.fold_in(own, position), (parts,), jnp.float32, smallest / len(cuts), largest / len(cuts)))
        gain = gain * jnp.repeat(draws, dims[position] // parts).reshape([-1 if axis == position else 1 for axis in range(len(dims))])
    return gain


def bell_draw(own_key, extent, scale, limit, cuts=(), dtype=jnp.bfloat16):
    entries = scale * jax.random.normal(own_key, extent, jnp.float32)
    if cuts:
        entries = entries * block_scale(own_key, extent, cuts, -0.22, 0.18)
    return jnp.clip(entries, -limit, limit).astype(dtype)


def setup_inputs(seed: int = 0) -> dict:
    key_of = jax.random.split(jax.random.key(seed), 7)
    return {
        "fields": bell_draw(key_of[0], (MEMBERS, NROWS, NLON), 2.0, 8.0, ((0, 32), (1, 16)), jnp.float32),
        "forcing": jnp.clip(2.0 + 6.0 * jax.random.uniform(key_of[1], (NROWS, NLON), jnp.float32) ** block_scale(key_of[1], (NROWS, NLON), ((0, 16),), -0.2, 0.2), 2.0, 8.0),
        "obs_cell": touch_ends(jax.random.randint(key_of[2], (N_LAT, PATCHES_STRIP, OBS), 0, PATCH_CELLS), jax.random.fold_in(key_of[2], 1), 0, PATCH_CELLS - 1).astype(jnp.int32),
        "obs_count": draw_obs_count(jax.random.fold_in(key_of[6], 71), 0),
        "obs_value": bell_draw(key_of[4], (N_LAT, PATCHES_STRIP, OBS), 3.0, 12.0, ((0, 16), (1, 32)), jnp.float32),
        "obs_var": jnp.clip(jnp.exp(math.log(1.0) - 1.3862944 * jax.random.uniform(key_of[5], (N_LAT, PATCHES_STRIP, OBS), jnp.float32) ** block_scale(key_of[5], (N_LAT, PATCHES_STRIP, OBS), ((0, 16), (1, 32)), -0.2, 0.2)), 0.25, 1.0),
    }


TIME_STEP = 0.05
LAT_MIXING = 4.0

def advance(middle, upper, lower, forcing):
    eastern = jnp.roll(middle, -1, axis=2)
    western = jnp.roll(middle, 1, axis=2)
    far_west = jnp.roll(middle, 2, axis=2)
    tendency = (eastern - far_west) * western - middle + forcing + LAT_MIXING * (upper + lower - 2.0 * middle)
    return middle + TIME_STEP * tendency

def analyse(patch_cells, observed, live_count, values, variances):
    members = patch_cells.shape[1]
    anomalies = patch_cells - jnp.mean(patch_cells, axis=1, keepdims=True)
    mean_obs = jnp.mean(observed, axis=1, keepdims=True)
    live = (jnp.arange(observed.shape[0]).astype(jnp.int32) < live_count)[:, None]
    obs_anom = jnp.where(live, observed - mean_obs, jnp.float32(0.0))
    gram = jnp.dot(obs_anom, obs_anom.T, precision=lax.Precision.HIGHEST) / (members - 1)
    gram = gram + jnp.diag(jnp.where(live[:, 0], variances, jnp.float32(1.0)))
    innovation = jnp.where(live, values[:, None] - mean_obs, jnp.float32(0.0))
    target = innovation - 0.5 * obs_anom
    factor = jnp.linalg.cholesky(gram)
    solved = jax.scipy.linalg.cho_solve((factor, True), target)
    cross = jnp.dot(anomalies, obs_anom.T, precision=lax.Precision.HIGHEST) / (members - 1)
    return patch_cells + jnp.dot(cross, solved, precision=lax.Precision.HIGHEST)

def reference(fields, forcing, obs_cell, obs_count, obs_value, obs_var):
    current = fields
    for repeat_index in range(STEPS):
        padded = jnp.pad(current, ((0, 0), (1, 1), (0, 0)))
        current = advance(current, padded[:, 2:], padded[:, :-2], forcing)
    members = current.shape[0]
    total_patches = N_LAT * PATCHES_STRIP
    patches = current.reshape(members, total_patches, PATCH_CELLS).transpose(1, 2, 0)

    def one_patch(items):
        patch_cells, cell_index, live_count, values, variances = items
        observed = jnp.take(patch_cells, cell_index, axis=0)
        return analyse(patch_cells, observed, live_count, values, variances)
    result = lax.map(one_patch, (patches, obs_cell.reshape(total_patches, OBS), obs_count.reshape(total_patches), obs_value.reshape(total_patches, OBS), obs_var.reshape(total_patches, OBS)))
    return result.transpose(2, 0, 1).reshape(members, NROWS, NLON)
```

```python
import functools

import jax
import jax.numpy as jnp
from jax import lax
from jax.experimental import pallas as pl
from jax.experimental.pallas import tpu as pltpu
from jax.sharding import PartitionSpec as P

CELLS = 64
STEPS = 4
TIME_STEP = 0.05
LAT_MIXING = 4.0
NEAR = 8
FAR = 4
HIGHEST = lax.Precision.HIGHEST
LANES = 128
NEAR_GROUPS = [[hi * NEAR + near for near in range(NEAR)] for hi in range(FAR)]
FAR_GROUPS = [[hi * NEAR + near for hi in range(FAR)] for near in range(NEAR)]


def low_half(shape):
    return lax.broadcasted_iota(jnp.int32, shape, 1) < CELLS


def halves(left, left_half, right, right_half):
    left = left if left_half == 0 else pltpu.roll(left, CELLS, 1)
    right = right if right_half == 1 else pltpu.roll(right, CELLS, 1)
    return jnp.where(low_half(left.shape), left, right)


def pack_kernel(fields, forcing, top, bottom):
    members = fields.shape[0]
    for out, start in ((top, 0), (bottom, STEPS)):
        for row in range(STEPS):
            out[pl.ds(row * members, members), :] = fields[:, start + row, :]
        edge = forcing[pl.ds(start, STEPS), :]
        out[pl.ds(STEPS * members, 2 * STEPS), :] = jnp.concatenate([edge, edge], axis=0)


def observe_kernel(scalars, cells, values, variances, out):
    slots = values.shape[2]
    live = lax.broadcasted_iota(jnp.int32, (1, slots), 1) < scalars[1]
    weight = jnp.where(live, 1.0 / variances[0], 0.0)
    scaled = weight * values[0]
    mine = cells[0, pl.ds(scalars[0], 1), :]
    cell = lax.broadcasted_iota(jnp.int32, (2 * CELLS, slots), 0) % CELLS
    hit = jnp.where(cell == mine, 1.0, 0.0)
    row = lax.broadcasted_iota(jnp.int32, (8, slots), 0)
    terms = jnp.where(row == 0, weight, jnp.where(row == 1, scaled, 0.0))
    sums = lax.dot_general(
        terms, hit, (((1,), (1,)), ((), ())), precision=HIGHEST, preferred_element_type=jnp.float32
    )
    both = jnp.where(low_half((1, LANES)), sums[0:1], sums[1:2])
    out[...] = jnp.broadcast_to(both, (8, LANES))


def forecast_kernel(last_strip, scalars, before, top, bottom, after, out):
    members = out.shape[1]
    strip = scalars[2]
    sources = [before] * STEPS + [top] * STEPS + [bottom] * STEPS + [after] * STEPS
    for tile in range(members // 8):
        rows = [
            source[pl.ds((place % STEPS) * members + tile * 8, 8), :]
            for place, source in enumerate(sources)
        ]
        for step in range(STEPS):
            updated = []
            for inner in range(1, len(rows) - 1):
                place = step + inner
                here = rows[inner]
                force = sources[place][pl.ds(STEPS * members + place % STEPS, 1), :]
                eastern = pltpu.roll(here, here.shape[1] - 1, 1)
                western = pltpu.roll(here, 1, 1)
                far_west = pltpu.roll(here, 2, 1)
                tendency = (
                    (eastern - far_west) * western
                    - here
                    + force
                    + LAT_MIXING * (rows[inner - 1] + rows[inner + 1] - 2.0 * here)
                )
                value = here + TIME_STEP * tendency
                if place < STEPS:
                    value = jnp.where(strip == 0, 0.0, value)
                if place >= 3 * STEPS:
                    value = jnp.where(strip == last_strip, 0.0, value)
                updated.append(value)
            rows = updated
        for near in range(NEAR):
            block = near % 4
            lanes = slice(block // 2 * LANES, block // 2 * LANES + LANES)
            parts = [rows[2 * hi + near // 4][:, lanes] for hi in range(FAR)]
            half = block % 2
            out[near, pl.ds(tile * 8, 8), pl.ds(0, LANES)] = halves(parts[0], half, parts[1], half)
            out[near, pl.ds(tile * 8, 8), pl.ds(LANES, LANES)] = halves(parts[2], half, parts[3], half)


def fold(square):
    return jnp.where(low_half((CELLS, LANES)), square[:CELLS], square[CELLS:])


def moments_kernel(states, observed, out):
    lines = []
    for half in range(2):
        block = states[:, pl.ds(half * LANES, LANES)]
        mean = jnp.sum(block, axis=0, keepdims=True) / block.shape[0]
        centred = block - mean
        square = lax.dot_general(
            centred, centred, (((0,), (0,)), ((), ())), precision=HIGHEST, preferred_element_type=jnp.float32
        )
        folded = fold(square)
        for hi in range(FAR):
            out[hi, pl.ds(half * CELLS, CELLS), :] = folded
        lines.append(mean)
    row = lax.broadcasted_iota(jnp.int32, (8, LANES), 0)
    tail = jnp.where(row == 0, lines[0], jnp.where(row == 1, lines[1], observed[...]))
    for hi in range(FAR):
        out[hi, pl.ds(LANES, 8), :] = tail


def eliminate(systems):
    row = lax.broadcasted_iota(jnp.int32, (8, LANES), 0)
    for pivot in range(CELLS):
        tile, line = divmod(pivot, 8)
        for system in systems:
            factors = [jnp.broadcast_to(part[:, pivot:pivot + 1], (8, LANES)) for part in system]
            lead = jnp.broadcast_to(system[tile][line:line + 1, :], (8, LANES))
            lead = lead / jnp.broadcast_to(factors[tile][line:line + 1, :], (8, LANES))
            for place in range(8):
                rest = system[place] - factors[place] * lead
                system[place] = jnp.where(row == line, lead, rest) if place == tile else rest
    return systems


def analyse_kernel(received, states, out, gains):
    group = states.shape[0]
    members = FAR * group
    low = low_half((CELLS, LANES))
    means, covariances = [], []
    for half in range(2):
        means_far = [received[hi, pl.ds(LANES + half, 1), :] for hi in range(FAR)]
        mean = (means_far[0] + means_far[1] + means_far[2] + means_far[3]) / FAR
        row = lax.broadcasted_iota(jnp.int32, (8, LANES), 0)
        offsets = jnp.zeros((8, LANES), jnp.float32)
        for hi in range(FAR):
            offsets = jnp.where(row == hi, means_far[hi] - mean, offsets)
        between = lax.dot_general(
            offsets, offsets, (((0,), (0,)), ((), ())), precision=HIGHEST, preferred_element_type=jnp.float32
        )
        total = group * fold(between)
        for hi in range(FAR):
            total = total + received[hi, pl.ds(half * CELLS, CELLS), :]
        means.append(mean)
        covariances.append(total / (members - 1))
    observed = [received[hi, pl.ds(LANES + 2, 1), :] for hi in range(FAR)]
    diagonal = lax.broadcasted_iota(jnp.int32, (CELLS, LANES), 0) == lax.broadcasted_iota(
        jnp.int32, (CELLS, LANES), 1
    )
    systems = []
    for patch in range(FAR):
        pair = covariances[patch // 2]
        twice = halves(pair, patch % 2, pair, patch % 2)
        scale = jnp.where(low_half((1, LANES)), observed[patch], 1.0)
        system = twice * scale + jnp.where(diagonal, 1.0, 0.0)
        systems.append([system[8 * tile:8 * tile + 8] for tile in range(8)])
    eliminate(systems)
    gains[...] = jnp.zeros(gains.shape, jnp.float32)
    for patch in range(FAR):
        for tile in range(8):
            block = systems[patch][tile]
            if patch % 2 == 0:
                block = pltpu.roll(block, CELLS, 1)
            keep = low_half((8, LANES)) if patch % 2 == 0 else jnp.logical_not(low_half((8, LANES)))
            rows = pl.ds(patch * CELLS + 8 * tile, 8)
            gains[rows, pl.ds(patch // 2 * LANES, LANES)] = jnp.where(keep, block, 0.0)
    for half in range(2):
        first, second = observed[2 * half], observed[2 * half + 1]
        weight = halves(first, 0, second, 0)
        source = halves(first, 1, second, 1)
        block = states[:, pl.ds(half * LANES, LANES)]
        mean = means[half]
        residual = (source - weight * mean) - (0.5 * weight) * (block - mean)
        square = gains[pl.ds(half * LANES, LANES), pl.ds(half * LANES, LANES)]
        out[:, pl.ds(half * LANES, LANES)] = block + jnp.dot(
            residual, square, precision=HIGHEST, preferred_element_type=jnp.float32
        )


def unpack_kernel(arrived, out):
    for row in range(out.shape[1]):
        hi, side = divmod(row, 2)
        lanes = pl.ds(hi // 2 * LANES, LANES)
        for pair in range(2):
            near = 4 * side + 2 * pair
            joined = halves(arrived[near, :, lanes], hi % 2, arrived[near + 1, :, lanes], hi % 2)
            out[:, row, pl.ds(pair * LANES, LANES)] = joined


VMEM = pl.BlockSpec(memory_space=pltpu.VMEM)
SMEM = pl.BlockSpec(memory_space=pltpu.SMEM)


def call(kernel, outs, in_specs, args, scratch=(), flops=1_000_000):
    many = isinstance(outs, list)
    shapes = [jax.ShapeDtypeStruct(s, jnp.float32) for s in (outs if many else [outs])]
    return pl.pallas_call(
        kernel,
        out_shape=shapes if many else shapes[0],
        in_specs=in_specs,
        out_specs=[VMEM] * len(shapes) if many else VMEM,
        scratch_shapes=list(scratch),
        compiler_params=pltpu.CompilerParams(vmem_limit_bytes=8 * 1024 * 1024),
        cost_estimate=pl.CostEstimate(flops=flops, bytes_accessed=500_000, transcendentals=0),
    )(*args)


def local(fields, forcing, obs_cell, obs_count, obs_value, obs_var):
    members, rows, lon = fields.shape
    strips = lax.axis_size("lat")
    scalars = jnp.stack([lax.axis_index("mem"), obs_count[0, 0], lax.axis_index("lat")]).astype(jnp.int32)
    height = STEPS * members + 2 * STEPS
    top, bottom = call(pack_kernel, [(height, lon)] * 2, [VMEM, VMEM], (fields, forcing))
    up = [(i, i + 1) for i in range(strips - 1)]
    down = [(j, i) for i, j in up]
    before = lax.ppermute(bottom, "lat", up)
    after = lax.ppermute(top, "lat", down)
    observed = call(observe_kernel, (8, LANES), [SMEM, VMEM, VMEM, VMEM], (scalars, obs_cell, obs_value, obs_var))
    states = call(
        functools.partial(forecast_kernel, strips - 1),
        (NEAR, members, lon),
        [SMEM, VMEM, VMEM, VMEM, VMEM],
        (scalars, before, top, bottom, after),
    )
    states = lax.all_to_all(states, "mem", 0, 0, axis_index_groups=NEAR_GROUPS, tiled=True)
    states = states.reshape(NEAR * members, lon)
    partial = call(moments_kernel, (FAR, LANES + 8, LANES), [VMEM, VMEM], (states, observed))
    received = lax.all_to_all(partial, "mem", 0, 0, axis_index_groups=FAR_GROUPS, tiled=True)
    result = call(
        analyse_kernel, states.shape, [VMEM, VMEM], (received, states), [pltpu.VMEM((2 * LANES, 2 * LANES), jnp.float32)]
    )
    result = result.reshape(NEAR, members, lon)
    result = lax.all_to_all(result, "mem", 0, 0, axis_index_groups=NEAR_GROUPS, tiled=True)
    return call(unpack_kernel, (members, rows, lon), [VMEM], (result,))


def solution(mesh):
    placed = (
        P("mem", "lat", None),
        P("lat", None),
        P("lat", None, None),
        P("lat", "mem"),
        P("lat", "mem", None),
        P("lat", "mem", None),
    )
    return jax.shard_map(local, mesh=mesh, in_specs=placed, out_specs=P("mem", "lat", None), check_vma=False)
```

```python
import functools

import jax
import jax.numpy as jnp
from jax import lax
from jax.experimental import pallas as pl
from jax.experimental.pallas import tpu as pltpu
from jax.sharding import PartitionSpec as P

CELLS = 64
STEPS = 4
TIME_STEP = 0.05
LAT_MIXING = 4.0
NEAR = 8
FAR = 4
HIGHEST = lax.Precision.HIGHEST
LANES = 128
NEAR_GROUPS = [[hi * NEAR + near for near in range(NEAR)] for hi in range(FAR)]
FAR_GROUPS = [[hi * NEAR + near for hi in range(FAR)] for near in range(NEAR)]


def low_half(shape):
    return lax.broadcasted_iota(jnp.int32, shape, 1) < CELLS


def halves(left, left_half, right, right_half):
    left = left if left_half == 0 else pltpu.roll(left, CELLS, 1)
    right = right if right_half == 1 else pltpu.roll(right, CELLS, 1)
    return jnp.where(low_half(left.shape), left, right)


def pack_kernel(fields, forcing, top, bottom, held, edges, sems):
    members = fields.shape[0]
    copies = [pltpu.make_async_copy(fields, held, sems.at[0]), pltpu.make_async_copy(forcing, edges, sems.at[1])]
    for copy in copies:
        copy.start()
    for copy in copies:
        copy.wait()
    for out, start in ((bottom, STEPS), (top, 0)):
        for row in range(STEPS):
            out[pl.ds(row * members, members), :] = held[:, start + row, :]
        edge = edges[pl.ds(start, STEPS), :]
        out[pl.ds(STEPS * members, 2 * STEPS), :] = jnp.concatenate([edge, edge], axis=0)


def observe_kernel(scalars, cells, values, variances, out):
    slots = values.shape[2]
    live = lax.broadcasted_iota(jnp.int32, (1, slots), 1) < scalars[1]
    weight = jnp.where(live, 1.0 / variances[0], 0.0)
    scaled = weight * values[0]
    mine = cells[0, pl.ds(scalars[0], 1), :]
    cell = lax.broadcasted_iota(jnp.int32, (2 * CELLS, slots), 0) % CELLS
    hit = jnp.where(cell == mine, 1.0, 0.0)
    row = lax.broadcasted_iota(jnp.int32, (8, slots), 0)
    terms = jnp.where(row == 0, weight, jnp.where(row == 1, scaled, 0.0))
    sums = lax.dot_general(
        terms, hit, (((1,), (1,)), ((), ())), precision=HIGHEST, preferred_element_type=jnp.float32
    )
    both = jnp.where(low_half((1, LANES)), sums[0:1], sums[1:2])
    out[...] = jnp.broadcast_to(both, (8, LANES))


def step_rows(rows, places, forces, strip, last_strip):
    updated = {}
    for place in places:
        here = rows[place]
        eastern = pltpu.roll(here, here.shape[1] - 1, 1)
        western = pltpu.roll(here, 1, 1)
        far_west = pltpu.roll(here, 2, 1)
        tendency = (
            (eastern - far_west) * western
            - here
            + forces(place)
            + LAT_MIXING * (rows[place - 1] + rows[place + 1] - 2.0 * here)
        )
        value = here + TIME_STEP * tendency
        if place < STEPS:
            value = jnp.where(strip == 0, 0.0, value)
        if place >= 3 * STEPS:
            value = jnp.where(strip == last_strip, 0.0, value)
        updated[place] = value
    return updated


def spread_patches(out, lanes_at, tile, rows):
    for near in range(NEAR):
        block = near % 4
        lanes = slice(block // 2 * LANES, block // 2 * LANES + LANES)
        first, second = rows[near // 4][:, lanes], rows[2 + near // 4][:, lanes]
        joined = halves(first, block % 2, second, block % 2)
        out[near, pl.ds(tile * 8, 8), pl.ds(lanes_at, LANES)] = joined


def early_kernel(last_strip, scalars, before, top, bottom, out, kept):
    members = out.shape[1]
    strip = scalars[2]
    sources = [before, top, bottom]

    def forces(place):
        return sources[place // STEPS][pl.ds(STEPS * members + place % STEPS, 1), :]

    for tile in range(members // 8):
        rows = {
            place: sources[place // STEPS][pl.ds((place % STEPS) * members + tile * 8, 8), :]
            for place in range(3 * STEPS)
        }
        for step in range(STEPS):
            rows = step_rows(rows, range(1 + step, 11 - step), forces, strip, last_strip)
            if step < STEPS - 1:
                for place in range(2):
                    kept[2 * step + place, pl.ds(tile * 8, 8), :] = rows[9 - step + place]
        spread_patches(out, 0, tile, [rows[place] for place in range(4, 8)])


def late_kernel(last_strip, scalars, bottom, after, kept, early, out):
    members = out.shape[1]
    strip = scalars[2]
    sources = [None, None, bottom, after]

    def forces(place):
        return sources[place // STEPS][pl.ds(STEPS * members + place % STEPS, 1), :]

    out[:, :, pl.ds(0, LANES)] = early[...]
    for tile in range(members // 8):
        rows = {
            place: sources[place // STEPS][pl.ds((place % STEPS) * members + tile * 8, 8), :]
            for place in range(10, 16)
        }
        for step in range(STEPS):
            if step > 0:
                for place in range(2):
                    rows[10 - step + place] = kept[2 * step - 2 + place, pl.ds(tile * 8, 8), :]
            rows = step_rows(rows, range(11 - step, 15 - step), forces, strip, last_strip)
        spread_patches(out, LANES, tile, [rows[place] for place in range(8, 12)])


def fold(square):
    return jnp.where(low_half((CELLS, LANES)), square[:CELLS], square[CELLS:])


def unfold(pair):
    low = low_half(pair.shape)
    return jnp.concatenate([jnp.where(low, pair, 0.0), jnp.where(low, 0.0, pair)], axis=0)


def places(shape):
    row = lax.broadcasted_iota(jnp.int32, shape, 0)
    return row, lax.broadcasted_iota(jnp.int32, shape, 1) % CELLS


def pack_symmetric(pair):
    side = CELLS // 2
    row, lane = places((side, LANES))
    take_upper = (lane >= side) & (row > lane - side)
    packed = jnp.where(take_upper, pltpu.roll(pair[:side], side, 1), pair[side:])
    return packed, jnp.sum(jnp.where(row == lane, pair[:side], 0.0), axis=0, keepdims=True)


def unpack_symmetric(packed, diagonals):
    side = CELLS // 2
    across = [halves(packed[0], half, packed[1], half) for half in range(2)]
    stacked = []
    for block in across:
        stacked += [pltpu.roll(block, LANES - side, 1), block]
    turned = jnp.concatenate(stacked, axis=0).T
    row, lane = places((CELLS, LANES))
    direct = ((lane < side) & (row > lane)) | ((lane >= side) & (row >= side) & (row <= lane))
    pairs = []
    for half in range(2):
        straight = jnp.concatenate([pltpu.roll(packed[half], LANES - side, 1), packed[half]], axis=0)
        full = jnp.where(direct, straight, turned[half * CELLS:(half + 1) * CELLS])
        pairs.append(jnp.where((row == lane) & (row < side), diagonals[half], full))
    return pairs


def moments_kernel(states, observed, out):
    lines = []
    for half in range(2):
        block = states[:, pl.ds(half * LANES, LANES)]
        mean = jnp.sum(block, axis=0, keepdims=True) / block.shape[0]
        centred = block - mean
        square = lax.dot_general(
            centred, centred, (((0,), (0,)), ((), ())), precision=HIGHEST, preferred_element_type=jnp.float32
        )
        packed, diagonal = pack_symmetric(fold(square))
        for hi in range(FAR):
            out[hi, pl.ds(half * CELLS // 2, CELLS // 2), :] = packed
        lines += [mean, diagonal]
    row = lax.broadcasted_iota(jnp.int32, (8, LANES), 0)
    tail = observed[...]
    for place, line in enumerate(lines):
        tail = jnp.where(row == place, line, tail)
    for hi in range(FAR):
        out[hi, pl.ds(CELLS, 8), :] = tail


def invert(pairs):
    row, lane = places((8, LANES))
    base = jnp.where(low_half((8, LANES)), 0, CELLS)

    def spread(block, line):
        return jnp.broadcast_to(block[line:line + 1, :], (8, LANES))

    for tile in range(8):
        inside = lane // 8 == tile
        identity = jnp.where(lane == row + 8 * tile, 1.0, 0.0)
        columns = [
            [
                [
                    jnp.take_along_axis(part, base + (8 * tile + c), axis=1, mode="promise_in_bounds")
                    for c in range(8)
                ]
                for part in pair
            ]
            for pair in pairs
        ]
        inverses = [list(factors[tile]) for factors in columns]
        for line in range(8):
            for inverse in inverses:
                reciprocal = 1.0 / spread(inverse[line], line)
                for c in range(8):
                    if c != line:
                        lead = spread(inverse[c], line) * reciprocal
                        inverse[c] = jnp.where(row == line, lead, inverse[c] - inverse[line] * lead)
                inverse[line] = jnp.where(row == line, reciprocal, -inverse[line] * reciprocal)
        for pair, factors, inverse in zip(pairs, columns, inverses):
            block = jnp.where(inside, identity, pair[tile])
            lead = inverse[0] * spread(block, 0)
            for c in range(1, 8):
                lead = lead + inverse[c] * spread(block, c)
            pair[tile] = lead
            leads = [spread(lead, c) for c in range(8)]
            for place in range(8):
                if place != tile:
                    rest = jnp.where(inside, 0.0, pair[place])
                    for c in range(8):
                        rest = rest - factors[place][c] * leads[c]
                    pair[place] = rest


def analyse_kernel(received, states, out):
    group = states.shape[0]
    members = FAR * group
    side = CELLS // 2

    def line(hi, place):
        return received[hi, pl.ds(CELLS + place, 1), :]

    def total(part):
        return part(0) + part(1) + part(2) + part(3)

    packed = [total(lambda hi: received[hi, pl.ds(half * side, side), :]) for half in range(2)]
    within = unpack_symmetric(packed, [total(lambda hi: line(hi, 2 * half + 1)) for half in range(2)])
    row, lane = places((CELLS, LANES))
    identity = jnp.where(row == lane, 1.0, 0.0)
    means, weights, shifts, pairs = [], [], [], []
    for half in range(2):
        mean = total(lambda hi: line(hi, 2 * half)) / FAR
        which = lax.broadcasted_iota(jnp.int32, (8, LANES), 0)
        offsets = jnp.zeros((8, LANES), jnp.float32)
        for hi in range(FAR):
            offsets = jnp.where(which == hi, line(hi, 2 * half) - mean, offsets)
        between = lax.dot_general(
            offsets, offsets, (((0,), (0,)), ((), ())), precision=HIGHEST, preferred_element_type=jnp.float32
        )
        covariance = (within[half] + group * fold(between)) / (members - 1)
        first, second = line(2 * half, 4), line(2 * half + 1, 4)
        weight = halves(first, 0, second, 0)
        shift = halves(first, 1, second, 1) - weight * mean
        shift = jnp.dot(
            jnp.broadcast_to(shift, (8, LANES)),
            unfold(covariance),
            precision=HIGHEST,
            preferred_element_type=jnp.float32,
        )
        system = covariance * weight + identity
        means.append(mean)
        shifts.append(shift[:1])
        pairs.append([system[8 * tile:8 * tile + 8] for tile in range(8)])
    invert(pairs)
    for half in range(2):
        block = states[:, pl.ds(half * LANES, LANES)]
        spread = 0.5 * (block - means[half])
        gain = unfold(jnp.concatenate(pairs[half], axis=0))
        out[:, pl.ds(half * LANES, LANES)] = (block - spread) + lax.dot_general(
            spread + shifts[half],
            gain,
            (((1,), (1,)), ((), ())),
            precision=HIGHEST,
            preferred_element_type=jnp.float32,
        )


def unpack_kernel(arrived, out):
    for row in range(out.shape[1]):
        hi, side = divmod(row, 2)
        lanes = pl.ds(hi // 2 * LANES, LANES)
        for pair in range(2):
            near = 4 * side + 2 * pair
            joined = halves(arrived[near, :, lanes], hi % 2, arrived[near + 1, :, lanes], hi % 2)
            out[:, row, pl.ds(pair * LANES, LANES)] = joined


VMEM = pl.BlockSpec(memory_space=pltpu.VMEM)
SMEM = pl.BlockSpec(memory_space=pltpu.SMEM)
HBM = pl.BlockSpec(memory_space=pltpu.HBM)


def call(kernel, outs, in_specs, args, scratch=(), flops=1_000_000):
    many = isinstance(outs, list)
    shapes = [jax.ShapeDtypeStruct(s, jnp.float32) for s in (outs if many else [outs])]
    return pl.pallas_call(
        kernel,
        out_shape=shapes if many else shapes[0],
        in_specs=in_specs,
        out_specs=[VMEM] * len(shapes) if many else VMEM,
        scratch_shapes=list(scratch),
        compiler_params=pltpu.CompilerParams(vmem_limit_bytes=8 * 1024 * 1024),
        cost_estimate=pl.CostEstimate(flops=flops, bytes_accessed=500_000, transcendentals=0),
    )(*args)


def local(fields, forcing, obs_cell, obs_count, obs_value, obs_var):
    members, rows, lon = fields.shape
    strips = lax.axis_size("lat")
    scalars = jnp.stack([lax.axis_index("mem"), obs_count[0, 0], lax.axis_index("lat")]).astype(jnp.int32)
    height = STEPS * members + 2 * STEPS
    top, bottom = call(
        pack_kernel,
        [(height, lon)] * 2,
        [HBM, HBM],
        (fields, forcing),
        [pltpu.VMEM(fields.shape, jnp.float32), pltpu.VMEM(forcing.shape, jnp.float32), pltpu.SemaphoreType.DMA((2,))],
    )
    up = [(i, i + 1) for i in range(strips - 1)]
    down = [(j, i) for i, j in up]
    before = lax.ppermute(bottom, "lat", up)
    after = lax.ppermute(top, "lat", down)
    observed = call(observe_kernel, (8, LANES), [SMEM, VMEM, VMEM, VMEM], (scalars, obs_cell, obs_value, obs_var))
    early, kept = call(
        functools.partial(early_kernel, strips - 1),
        [(NEAR, members, LANES), (6, members, lon)],
        [SMEM, VMEM, VMEM, VMEM],
        (scalars, before, top, bottom),
        flops=10_000_000,
    )
    states = call(
        functools.partial(late_kernel, strips - 1),
        (NEAR, members, lon),
        [SMEM, VMEM, VMEM, VMEM, VMEM],
        (scalars, bottom, after, kept, early),
    )
    states = lax.all_to_all(states, "mem", 0, 0, axis_index_groups=NEAR_GROUPS, tiled=True)
    states = states.reshape(NEAR * members, lon)
    partial = call(moments_kernel, (FAR, CELLS + 8, LANES), [VMEM, VMEM], (states, observed))
    received = lax.all_to_all(partial, "mem", 0, 0, axis_index_groups=FAR_GROUPS, tiled=True)
    result = call(analyse_kernel, states.shape, [VMEM, VMEM], (received, states))
    result = result.reshape(NEAR, members, lon)
    result = lax.all_to_all(result, "mem", 0, 0, axis_index_groups=NEAR_GROUPS, tiled=True)
    return call(unpack_kernel, (members, rows, lon), [VMEM], (result,))


def solution(mesh):
    placed = (
        P("mem", "lat", None),
        P("lat", None),
        P("lat", None, None),
        P("lat", "mem"),
        P("lat", "mem", None),
        P("lat", "mem", None),
    )
    return jax.shard_map(local, mesh=mesh, in_specs=placed, out_specs=P("mem", "lat", None), check_vma=False)
```

```python
import functools

import jax
import jax.numpy as jnp
from jax import lax
from jax.experimental import pallas as pl
from jax.experimental.pallas import tpu as pltpu
from jax.sharding import PartitionSpec as P

CELLS = 64
STEPS = 4
TIME_STEP = 0.05
LAT_MIXING = 4.0
NEAR = 8
FAR = 4
HIGHEST = lax.Precision.HIGHEST
LANES = 128
NEAR_GROUPS = [[hi * NEAR + near for near in range(NEAR)] for hi in range(FAR)]


def low_half(shape):
    return lax.broadcasted_iota(jnp.int32, shape, 1) < CELLS


def halves(left, left_half, right, right_half):
    left = left if left_half == 0 else pltpu.roll(left, CELLS, 1)
    right = right if right_half == 1 else pltpu.roll(right, CELLS, 1)
    return jnp.where(low_half(left.shape), left, right)


def pack_kernel(fields, forcing, top, bottom, held, edges, sems):
    members = fields.shape[0]
    copies = [pltpu.make_async_copy(fields, held, sems.at[0]), pltpu.make_async_copy(forcing, edges, sems.at[1])]
    for copy in copies:
        copy.start()
    for copy in copies:
        copy.wait()
    for out, start in ((bottom, STEPS), (top, 0)):
        for row in range(STEPS):
            out[pl.ds(row * members, members), :] = held[:, start + row, :]
        edge = edges[pl.ds(start, STEPS), :]
        out[pl.ds(STEPS * members, 2 * STEPS), :] = jnp.concatenate([edge, edge], axis=0)


def observe(scalars, cells, values, variances, out):
    slots = values.shape[2]
    live = lax.broadcasted_iota(jnp.int32, (1, slots), 1) < scalars[1]
    weight = jnp.where(live, 1.0 / variances[0], 0.0)
    scaled = weight * values[0]
    mine = cells[0, pl.ds(scalars[0], 1), :]
    cell = lax.broadcasted_iota(jnp.int32, (2 * CELLS, slots), 0) % CELLS
    hit = jnp.where(cell == mine, 1.0, 0.0)
    row = lax.broadcasted_iota(jnp.int32, (8, slots), 0)
    terms = jnp.where(row == 0, weight, jnp.where(row == 1, scaled, 0.0))
    sums = lax.dot_general(
        terms, hit, (((1,), (1,)), ((), ())), precision=HIGHEST, preferred_element_type=jnp.float32
    )
    both = jnp.where(low_half((1, LANES)), sums[0:1], sums[1:2])
    out[...] = jnp.broadcast_to(both, (8, LANES))


def step_rows(rows, places, forces, strip, last_strip):
    updated = {}
    for place in places:
        here = rows[place]
        eastern = pltpu.roll(here, here.shape[1] - 1, 1)
        western = pltpu.roll(here, 1, 1)
        far_west = pltpu.roll(here, 2, 1)
        tendency = (
            (eastern - far_west) * western
            - here
            + forces(place)
            + LAT_MIXING * (rows[place - 1] + rows[place + 1] - 2.0 * here)
        )
        value = here + TIME_STEP * tendency
        if place < STEPS:
            value = jnp.where(strip == 0, 0.0, value)
        if place >= 3 * STEPS:
            value = jnp.where(strip == last_strip, 0.0, value)
        updated[place] = value
    return updated


def spread_patches(out, lanes_at, tile, rows):
    for near in range(NEAR):
        block = near % 4
        lanes = slice(block // 2 * LANES, block // 2 * LANES + LANES)
        first, second = rows[near // 4][:, lanes], rows[2 + near // 4][:, lanes]
        joined = halves(first, block % 2, second, block % 2)
        out[near, pl.ds(tile * first.shape[0], first.shape[0]), pl.ds(lanes_at, LANES)] = joined


def early_kernel(last_strip, scalars, cells, values, variances, before, top, bottom, out, kept, observed):
    observe(scalars, cells, values, variances, observed)
    members = out.shape[1]
    strip = scalars[2]
    sources = [before, top, bottom]

    def forces(place):
        return sources[place // STEPS][pl.ds(STEPS * members + place % STEPS, 1), :]

    for tile in range(members // 32):
        rows = {
            place: sources[place // STEPS][pl.ds((place % STEPS) * members + tile * 32, 32), :]
            for place in range(3 * STEPS)
        }
        for step in range(STEPS):
            rows = step_rows(rows, range(1 + step, 11 - step), forces, strip, last_strip)
            if step < STEPS - 1:
                for place in range(2):
                    kept[2 * step + place, pl.ds(tile * 32, 32), :] = rows[9 - step + place]
        spread_patches(out, 0, tile, [rows[place] for place in range(4, 8)])


def late_kernel(last_strip, scalars, bottom, after, kept, early, out):
    members = out.shape[1]
    strip = scalars[2]
    sources = [None, None, bottom, after]

    def forces(place):
        return sources[place // STEPS][pl.ds(STEPS * members + place % STEPS, 1), :]

    out[:, :, pl.ds(0, LANES)] = early[...]
    for tile in range(members // 32):
        rows = {
            place: sources[place // STEPS][pl.ds((place % STEPS) * members + tile * 32, 32), :]
            for place in range(10, 16)
        }
        for step in range(STEPS):
            if step > 0:
                for place in range(2):
                    rows[10 - step + place] = kept[2 * step - 2 + place, pl.ds(tile * 32, 32), :]
            rows = step_rows(rows, range(11 - step, 15 - step), forces, strip, last_strip)
        spread_patches(out, LANES, tile, [rows[place] for place in range(8, 12)])


def fold(square):
    return jnp.where(low_half((CELLS, LANES)), square[:CELLS], square[CELLS:])


def unfold(pair):
    low = low_half(pair.shape)
    return jnp.concatenate([jnp.where(low, pair, 0.0), jnp.where(low, 0.0, pair)], axis=0)


def places(shape):
    row = lax.broadcasted_iota(jnp.int32, shape, 0)
    return row, lax.broadcasted_iota(jnp.int32, shape, 1) % CELLS


def pack_symmetric(pair):
    side = CELLS // 2
    row, lane = places((side, LANES))
    take_upper = (lane >= side) & (row > lane - side)
    packed = jnp.where(take_upper, pltpu.roll(pair[:side], side, 1), pair[side:])
    return packed, jnp.sum(jnp.where(row == lane, pair[:side], 0.0), axis=0, keepdims=True)


def unpack_symmetric(packed, diagonals):
    side = CELLS // 2
    across = [halves(packed[0], half, packed[1], half) for half in range(2)]
    stacked = []
    for block in across:
        stacked += [pltpu.roll(block, LANES - side, 1), block]
    turned = jnp.concatenate(stacked, axis=0).T
    row, lane = places((CELLS, LANES))
    direct = ((lane < side) & (row > lane)) | ((lane >= side) & (row >= side) & (row <= lane))
    pairs = []
    for half in range(2):
        straight = jnp.concatenate([pltpu.roll(packed[half], LANES - side, 1), packed[half]], axis=0)
        full = jnp.where(direct, straight, turned[half * CELLS:(half + 1) * CELLS])
        pairs.append(jnp.where((row == lane) & (row < side), diagonals[half], full))
    return pairs


def moments_kernel(states, observed, out):
    lines = []
    for half in range(2):
        block = states[:, pl.ds(half * LANES, LANES)]
        mean = jnp.sum(block, axis=0, keepdims=True) / block.shape[0]
        centred = block - mean
        square = lax.dot_general(
            centred, centred, (((0,), (0,)), ((), ())), precision=HIGHEST, preferred_element_type=jnp.float32
        )
        packed, diagonal = pack_symmetric(fold(square))
        out[pl.ds(half * CELLS // 2, CELLS // 2), :] = packed
        lines += [mean, diagonal]
    row = lax.broadcasted_iota(jnp.int32, (8, LANES), 0)
    tail = observed[...]
    for place, line in enumerate(lines):
        tail = jnp.where(row == place, line, tail)
    out[pl.ds(CELLS, 8), :] = tail


def invert(pairs):
    row, lane = places((8, LANES))
    base = jnp.where(low_half((8, LANES)), 0, CELLS)

    def spread(block, line):
        return jnp.broadcast_to(block[line:line + 1, :], (8, LANES))

    for tile in range(8):
        inside = lane // 8 == tile
        identity = jnp.where(lane == row + 8 * tile, 1.0, 0.0)
        near = (tile, (tile + 1) % 8)
        columns = [
            [
                [
                    jnp.take_along_axis(part, base + (8 * tile + c), axis=1, mode="promise_in_bounds")
                    for c in range(8)
                ]
                if place in near
                else None
                for place, part in enumerate(pair)
            ]
            for pair in pairs
        ]
        inverses = [list(factors[tile]) for factors in columns]
        for line in range(8):
            for inverse in inverses:
                reciprocal = 1.0 / spread(inverse[line], line)
                for c in range(8):
                    if c != line:
                        lead = spread(inverse[c], line) * reciprocal
                        inverse[c] = jnp.where(row == line, lead, inverse[c] - inverse[line] * lead)
                inverse[line] = jnp.where(row == line, reciprocal, -inverse[line] * reciprocal)
        for pair, factors, inverse in zip(pairs, columns, inverses):
            block = jnp.where(inside, identity, pair[tile])
            lead = inverse[0] * spread(block, 0)
            for c in range(1, 8):
                lead = lead + inverse[c] * spread(block, c)
            whole = jnp.concatenate(pair, axis=0)
            across = jnp.where(places((CELLS, LANES))[1] // 8 == tile, whole, 0.0)
            low = low_half((8, LANES))
            empty = jnp.zeros((8, LANES), jnp.float32)
            rows = [empty] * 16
            rows[tile] = jnp.where(low, lead, 0.0)
            rows[8 + tile] = jnp.where(low, 0.0, lead)
            product = jnp.dot(
                across, jnp.concatenate(rows, axis=0), precision=HIGHEST, preferred_element_type=jnp.float32
            )
            for place in range(8):
                if place not in near:
                    pair[place] = jnp.where(inside, 0.0, pair[place]) - product[8 * place:8 * place + 8]
            pair[tile] = lead
            leads = [spread(lead, c) for c in range(8)]
            for place in near:
                if place != tile:
                    rest = jnp.where(inside, 0.0, pair[place])
                    for c in range(8):
                        rest = rest - factors[place][c] * leads[c]
                    pair[place] = rest


def analyse_kernel(scalars, own, ahead1, ahead2, ahead3, states, out):
    group = states.shape[0]
    members = FAR * group
    side = CELLS // 2
    received = (own, ahead1, ahead2, ahead3)

    def line(back, place):
        return received[back][pl.ds(CELLS + place, 1), :]

    def observed(hi):
        back = (scalars[0] // NEAR + FAR - hi) % FAR
        value = line(0, 4)
        for place in range(1, FAR):
            value = jnp.where(back == place, line(place, 4), value)
        return value

    def total(part):
        return part(0) + part(1) + part(2) + part(3)

    packed = [total(lambda back: received[back][pl.ds(half * side, side), :]) for half in range(2)]
    within = unpack_symmetric(packed, [total(lambda hi: line(hi, 2 * half + 1)) for half in range(2)])
    row, lane = places((CELLS, LANES))
    identity = jnp.where(row == lane, 1.0, 0.0)
    means, weights, shifts, pairs = [], [], [], []
    for half in range(2):
        mean = total(lambda hi: line(hi, 2 * half)) / FAR
        which = lax.broadcasted_iota(jnp.int32, (8, LANES), 0)
        offsets = jnp.zeros((8, LANES), jnp.float32)
        for hi in range(FAR):
            offsets = jnp.where(which == hi, line(hi, 2 * half) - mean, offsets)
        between = lax.dot_general(
            offsets, offsets, (((0,), (0,)), ((), ())), precision=HIGHEST, preferred_element_type=jnp.float32
        )
        covariance = (within[half] + group * fold(between)) / (members - 1)
        first, second = observed(2 * half), observed(2 * half + 1)
        weight = halves(first, 0, second, 0)
        shift = halves(first, 1, second, 1) - weight * mean
        shift = jnp.dot(
            jnp.broadcast_to(shift, (8, LANES)),
            unfold(covariance),
            precision=HIGHEST,
            preferred_element_type=jnp.float32,
        )
        system = covariance * weight + identity
        means.append(mean)
        shifts.append(shift[:1])
        pairs.append([system[8 * tile:8 * tile + 8] for tile in range(8)])
    invert(pairs)
    for half in range(2):
        block = states[:, pl.ds(half * LANES, LANES)]
        spread = 0.5 * (block - means[half])
        gain = unfold(jnp.concatenate(pairs[half], axis=0))
        out[:, pl.ds(half * LANES, LANES)] = (block - spread) + lax.dot_general(
            spread + shifts[half],
            gain,
            (((1,), (1,)), ((), ())),
            precision=HIGHEST,
            preferred_element_type=jnp.float32,
        )


def unpack_kernel(arrived, out):
    for row in range(out.shape[1]):
        hi, side = divmod(row, 2)
        lanes = pl.ds(hi // 2 * LANES, LANES)
        for pair in range(2):
            near = 4 * side + 2 * pair
            joined = halves(arrived[near, :, lanes], hi % 2, arrived[near + 1, :, lanes], hi % 2)
            out[:, row, pl.ds(pair * LANES, LANES)] = joined


VMEM = pl.BlockSpec(memory_space=pltpu.VMEM)
SMEM = pl.BlockSpec(memory_space=pltpu.SMEM)
HBM = pl.BlockSpec(memory_space=pltpu.HBM)


def call(kernel, outs, in_specs, args, scratch=(), flops=1_000_000):
    many = isinstance(outs, list)
    shapes = [jax.ShapeDtypeStruct(s, jnp.float32) for s in (outs if many else [outs])]
    return pl.pallas_call(
        kernel,
        out_shape=shapes if many else shapes[0],
        in_specs=in_specs,
        out_specs=[VMEM] * len(shapes) if many else VMEM,
        scratch_shapes=list(scratch),
        compiler_params=pltpu.CompilerParams(vmem_limit_bytes=8 * 1024 * 1024),
        cost_estimate=pl.CostEstimate(flops=flops, bytes_accessed=500_000, transcendentals=0),
    )(*args)


def local(fields, forcing, obs_cell, obs_count, obs_value, obs_var):
    members, rows, lon = fields.shape
    strips = lax.axis_size("lat")
    scalars = jnp.stack([lax.axis_index("mem"), obs_count[0, 0], lax.axis_index("lat")]).astype(jnp.int32)
    height = STEPS * members + 2 * STEPS
    fields, forcing = (pltpu.with_memory_space_constraint(value, pltpu.HBM) for value in (fields, forcing))
    top, bottom = call(
        pack_kernel,
        [(height, lon)] * 2,
        [HBM, HBM],
        (fields, forcing),
        [pltpu.VMEM(fields.shape, jnp.float32), pltpu.VMEM(forcing.shape, jnp.float32), pltpu.SemaphoreType.DMA((2,))],
    )
    up = [(i, i + 1) for i in range(strips - 1)]
    down = [(j, i) for i, j in up]
    before = lax.ppermute(bottom, "lat", up)
    after = lax.ppermute(top, "lat", down)
    early, kept, observed = call(
        functools.partial(early_kernel, strips - 1),
        [(NEAR, members, LANES), (6, members, lon), (8, LANES)],
        [SMEM] + [VMEM] * 6,
        (scalars, obs_cell, obs_value, obs_var, before, top, bottom),
        flops=10_000_000,
    )
    states = call(
        functools.partial(late_kernel, strips - 1),
        (NEAR, members, lon),
        [SMEM, VMEM, VMEM, VMEM, VMEM],
        (scalars, bottom, after, kept, early),
    )
    states = lax.all_to_all(states, "mem", 0, 0, axis_index_groups=NEAR_GROUPS, tiled=True)
    states = states.reshape(NEAR * members, lon)
    partial = call(moments_kernel, (CELLS + 8, LANES), [VMEM, VMEM], (states, observed))
    size = FAR * NEAR
    onward = [(i, (i + NEAR) % size) for i in range(size)]
    ahead1 = lax.ppermute(partial, "mem", onward)
    ahead3 = lax.ppermute(partial, "mem", [(j, i) for i, j in onward])
    ahead2 = lax.ppermute(ahead1, "mem", onward)
    result = call(
        analyse_kernel,
        states.shape,
        [SMEM] + [VMEM] * (FAR + 1),
        (scalars, partial, ahead1, ahead2, ahead3, states),
    )
    result = result.reshape(NEAR, members, lon)
    result = lax.all_to_all(result, "mem", 0, 0, axis_index_groups=NEAR_GROUPS, tiled=True)
    return call(unpack_kernel, (members, rows, lon), [VMEM], (result,))


def solution(mesh):
    placed = (
        P("mem", "lat", None),
        P("lat", None),
        P("lat", None, None),
        P("lat", "mem"),
        P("lat", "mem", None),
        P("lat", "mem", None),
    )
    return jax.shard_map(local, mesh=mesh, in_specs=placed, out_specs=P("mem", "lat", None), check_vma=False)
```

```python
import functools

import jax
import jax.numpy as jnp
from jax import lax
from jax.experimental import pallas as pl
from jax.experimental.pallas import tpu as pltpu
from jax.sharding import PartitionSpec as P

CELLS = 64
STEPS = 4
TIME_STEP = 0.05
LAT_MIXING = 4.0
NEAR = 8
FAR = 4
HIGHEST = lax.Precision.HIGHEST
LANES = 128
NEAR_GROUPS = [[hi * NEAR + near for near in range(NEAR)] for hi in range(FAR)]


def low_half(shape):
    return lax.broadcasted_iota(jnp.int32, shape, 1) < CELLS


def halves(left, left_half, right, right_half):
    left = left if left_half == 0 else pltpu.roll(left, CELLS, 1)
    right = right if right_half == 1 else pltpu.roll(right, CELLS, 1)
    return jnp.where(low_half(left.shape), left, right)


def pack_kernel(fields, forcing, top, bottom, held, edges, sems):
    members = fields.shape[0]
    copies = [pltpu.make_async_copy(fields, held, sems.at[0]), pltpu.make_async_copy(forcing, edges, sems.at[1])]
    for copy in copies:
        copy.start()
    for copy in copies:
        copy.wait()
    for out, start in ((bottom, STEPS), (top, 0)):
        for row in range(STEPS):
            out[pl.ds(row * members, members), :] = held[:, start + row, :]
        edge = edges[pl.ds(start, STEPS), :]
        out[pl.ds(STEPS * members, 2 * STEPS), :] = jnp.concatenate([edge, edge], axis=0)


def observe(count, cells, values, variances, out):
    slots = values.shape[2]
    live = lax.broadcasted_iota(jnp.int32, (1, slots), 1) < count[...]
    weight = jnp.where(live, 1.0 / variances[0], 0.0)
    scaled = weight * values[0]
    mine = cells[0, pl.ds(lax.axis_index("mem"), 1), :]
    cell = lax.broadcasted_iota(jnp.int32, (2 * CELLS, slots), 0) % CELLS
    hit = jnp.where(cell == mine, 1.0, 0.0)
    row = lax.broadcasted_iota(jnp.int32, (8, slots), 0)
    terms = jnp.where(row == 0, weight, jnp.where(row == 1, scaled, 0.0))
    sums = lax.dot_general(
        terms, hit, (((1,), (1,)), ((), ())), precision=HIGHEST, preferred_element_type=jnp.float32
    )
    both = jnp.where(low_half((1, LANES)), sums[0:1], sums[1:2])
    out[...] = jnp.broadcast_to(both, (8, LANES))


def step_rows(rows, places, forces, strip, last_strip):
    updated = {}
    for place in places:
        here = rows[place]
        eastern = pltpu.roll(here, here.shape[1] - 1, 1)
        western = pltpu.roll(here, 1, 1)
        far_west = pltpu.roll(here, 2, 1)
        tendency = (
            (eastern - far_west) * western
            - here
            + forces(place)
            + LAT_MIXING * (rows[place - 1] + rows[place + 1] - 2.0 * here)
        )
        value = here + TIME_STEP * tendency
        if place < STEPS:
            value = jnp.where(strip == 0, 0.0, value)
        if place >= 3 * STEPS:
            value = jnp.where(strip == last_strip, 0.0, value)
        updated[place] = value
    return updated


def spread_patches(out, lanes_at, tile, rows):
    for near in range(NEAR):
        block = near % 4
        lanes = slice(block // 2 * LANES, block // 2 * LANES + LANES)
        first, second = rows[near // 4][:, lanes], rows[2 + near // 4][:, lanes]
        joined = halves(first, block % 2, second, block % 2)
        out[near, pl.ds(tile * first.shape[0], first.shape[0]), pl.ds(lanes_at, LANES)] = joined


def early_kernel(last_strip, count, cells, values, variances, before, top, bottom, out, kept, observed):
    observe(count, cells, values, variances, observed)
    members = out.shape[1]
    strip = lax.axis_index("lat")
    sources = [before, top, bottom]

    def forces(place):
        return sources[place // STEPS][pl.ds(STEPS * members + place % STEPS, 1), :]

    for tile in range(members // 32):
        rows = {
            place: sources[place // STEPS][pl.ds((place % STEPS) * members + tile * 32, 32), :]
            for place in range(3 * STEPS)
        }
        for step in range(STEPS):
            rows = step_rows(rows, range(1 + step, 11 - step), forces, strip, last_strip)
            if step < STEPS - 1:
                for place in range(2):
                    kept[2 * step + place, pl.ds(tile * 32, 32), :] = rows[9 - step + place]
        spread_patches(out, 0, tile, [rows[place] for place in range(4, 8)])


def late_kernel(last_strip, bottom, after, kept, early, out):
    members = out.shape[1]
    strip = lax.axis_index("lat")
    sources = [None, None, bottom, after]

    def forces(place):
        return sources[place // STEPS][pl.ds(STEPS * members + place % STEPS, 1), :]

    out[:, :, pl.ds(0, LANES)] = early[...]
    for tile in range(members // 32):
        rows = {
            place: sources[place // STEPS][pl.ds((place % STEPS) * members + tile * 32, 32), :]
            for place in range(10, 16)
        }
        for step in range(STEPS):
            if step > 0:
                for place in range(2):
                    rows[10 - step + place] = kept[2 * step - 2 + place, pl.ds(tile * 32, 32), :]
            rows = step_rows(rows, range(11 - step, 15 - step), forces, strip, last_strip)
        spread_patches(out, LANES, tile, [rows[place] for place in range(8, 12)])


def fold(square):
    return jnp.where(low_half((CELLS, LANES)), square[:CELLS], square[CELLS:])


def unfold(pair):
    low = low_half(pair.shape)
    return jnp.concatenate([jnp.where(low, pair, 0.0), jnp.where(low, 0.0, pair)], axis=0)


def places(shape):
    row = lax.broadcasted_iota(jnp.int32, shape, 0)
    return row, lax.broadcasted_iota(jnp.int32, shape, 1) % CELLS


def pack_symmetric(pair):
    side = CELLS // 2
    row, lane = places((side, LANES))
    take_upper = (lane >= side) & (row > lane - side)
    packed = jnp.where(take_upper, pltpu.roll(pair[:side], side, 1), pair[side:])
    return packed, jnp.sum(jnp.where(row == lane, pair[:side], 0.0), axis=0, keepdims=True)


def unpack_symmetric(packed, diagonals):
    side = CELLS // 2
    across = [halves(packed[0], half, packed[1], half) for half in range(2)]
    stacked = []
    for block in across:
        stacked += [pltpu.roll(block, LANES - side, 1), block]
    turned = jnp.concatenate(stacked, axis=0).T
    row, lane = places((CELLS, LANES))
    direct = ((lane < side) & (row > lane)) | ((lane >= side) & (row >= side) & (row <= lane))
    pairs = []
    for half in range(2):
        straight = jnp.concatenate([pltpu.roll(packed[half], LANES - side, 1), packed[half]], axis=0)
        full = jnp.where(direct, straight, turned[half * CELLS:(half + 1) * CELLS])
        pairs.append(jnp.where((row == lane) & (row < side), diagonals[half], full))
    return pairs


def moments_kernel(states, observed, out):
    lines = []
    for half in range(2):
        block = states[:, pl.ds(half * LANES, LANES)]
        mean = jnp.sum(block, axis=0, keepdims=True) / block.shape[0]
        centred = block - mean
        square = lax.dot_general(
            centred, centred, (((0,), (0,)), ((), ())), precision=HIGHEST, preferred_element_type=jnp.float32
        )
        packed, diagonal = pack_symmetric(fold(square))
        out[pl.ds(half * CELLS // 2, CELLS // 2), :] = packed
        lines += [mean, diagonal]
    row = lax.broadcasted_iota(jnp.int32, (8, LANES), 0)
    tail = observed[...]
    for place, line in enumerate(lines):
        tail = jnp.where(row == place, line, tail)
    out[pl.ds(CELLS, 8), :] = tail


def invert(pairs):
    row, lane = places((8, LANES))
    base = jnp.where(low_half((8, LANES)), 0, CELLS)

    def spread(block, line):
        return jnp.broadcast_to(block[line:line + 1, :], (8, LANES))

    for tile in range(8):
        inside = lane // 8 == tile
        identity = jnp.where(lane == row + 8 * tile, 1.0, 0.0)
        near = (tile, (tile + 1) % 8)
        columns = [
            [
                [
                    jnp.take_along_axis(part, base + (8 * tile + c), axis=1, mode="promise_in_bounds")
                    for c in range(8)
                ]
                if place in near
                else None
                for place, part in enumerate(pair)
            ]
            for pair in pairs
        ]
        inverses = [list(factors[tile]) for factors in columns]
        for line in range(8):
            for inverse in inverses:
                reciprocal = 1.0 / spread(inverse[line], line)
                for c in range(8):
                    if c != line:
                        lead = spread(inverse[c], line) * reciprocal
                        inverse[c] = jnp.where(row == line, lead, inverse[c] - inverse[line] * lead)
                inverse[line] = jnp.where(row == line, reciprocal, -inverse[line] * reciprocal)
        for pair, factors, inverse in zip(pairs, columns, inverses):
            block = jnp.where(inside, identity, pair[tile])
            lead = inverse[0] * spread(block, 0)
            for c in range(1, 8):
                lead = lead + inverse[c] * spread(block, c)
            whole = jnp.concatenate(pair, axis=0)
            across = jnp.where(places((CELLS, LANES))[1] // 8 == tile, whole, 0.0)
            low = low_half((8, LANES))
            empty = jnp.zeros((8, LANES), jnp.float32)
            rows = [empty] * 16
            rows[tile] = jnp.where(low, lead, 0.0)
            rows[8 + tile] = jnp.where(low, 0.0, lead)
            product = jnp.dot(
                across, jnp.concatenate(rows, axis=0), precision=HIGHEST, preferred_element_type=jnp.float32
            )
            for place in range(8):
                if place not in near:
                    pair[place] = jnp.where(inside, 0.0, pair[place]) - product[8 * place:8 * place + 8]
            pair[tile] = lead
            leads = [spread(lead, c) for c in range(8)]
            for place in near:
                if place != tile:
                    rest = jnp.where(inside, 0.0, pair[place])
                    for c in range(8):
                        rest = rest - factors[place][c] * leads[c]
                    pair[place] = rest


def analyse_kernel(received, states, out):
    group = states.shape[0]
    members = FAR * group
    side = CELLS // 2

    def line(hi, place):
        return received[hi // 2, pl.ds(CELLS + 8 * (hi % 2) + place, 1), :]

    def observed(hi):
        return line(hi, 4)

    def total(part):
        return part(0) + part(1) + part(2) + part(3)

    packed = [received[0, pl.ds(half * side, side), :] + received[1, pl.ds(half * side, side), :] for half in range(2)]
    within = unpack_symmetric(packed, [total(lambda hi: line(hi, 2 * half + 1)) for half in range(2)])
    row, lane = places((CELLS, LANES))
    identity = jnp.where(row == lane, 1.0, 0.0)
    means, weights, shifts, pairs = [], [], [], []
    for half in range(2):
        mean = total(lambda hi: line(hi, 2 * half)) / FAR
        which = lax.broadcasted_iota(jnp.int32, (8, LANES), 0)
        offsets = jnp.zeros((8, LANES), jnp.float32)
        for hi in range(FAR):
            offsets = jnp.where(which == hi, line(hi, 2 * half) - mean, offsets)
        between = lax.dot_general(
            offsets, offsets, (((0,), (0,)), ((), ())), precision=HIGHEST, preferred_element_type=jnp.float32
        )
        covariance = (within[half] + group * fold(between)) / (members - 1)
        first, second = observed(2 * half), observed(2 * half + 1)
        weight = halves(first, 0, second, 0)
        shift = halves(first, 1, second, 1) - weight * mean
        shift = jnp.dot(
            jnp.broadcast_to(shift, (8, LANES)),
            unfold(covariance),
            precision=HIGHEST,
            preferred_element_type=jnp.float32,
        )
        system = covariance * weight + identity
        means.append(mean)
        shifts.append(shift[:1])
        pairs.append([system[8 * tile:8 * tile + 8] for tile in range(8)])
    invert(pairs)
    for half in range(2):
        block = states[:, pl.ds(half * LANES, LANES)]
        spread = 0.5 * (block - means[half])
        gain = unfold(jnp.concatenate(pairs[half], axis=0))
        out[:, pl.ds(half * LANES, LANES)] = (block - spread) + lax.dot_general(
            spread + shifts[half],
            gain,
            (((1,), (1,)), ((), ())),
            precision=HIGHEST,
            preferred_element_type=jnp.float32,
        )


def unpack_kernel(arrived, out):
    for row in range(out.shape[1]):
        hi, side = divmod(row, 2)
        lanes = pl.ds(hi // 2 * LANES, LANES)
        for pair in range(2):
            near = 4 * side + 2 * pair
            joined = halves(arrived[near, :, lanes], hi % 2, arrived[near + 1, :, lanes], hi % 2)
            out[:, row, pl.ds(pair * LANES, LANES)] = joined


VMEM = pl.BlockSpec(memory_space=pltpu.VMEM)
HBM = pl.BlockSpec(memory_space=pltpu.HBM)


def call(kernel, outs, in_specs, args, scratch=(), flops=1_000_000):
    many = isinstance(outs, list)
    shapes = [jax.ShapeDtypeStruct(s, jnp.float32) for s in (outs if many else [outs])]
    return pl.pallas_call(
        kernel,
        out_shape=shapes if many else shapes[0],
        in_specs=in_specs,
        out_specs=[VMEM] * len(shapes) if many else VMEM,
        scratch_shapes=list(scratch),
        compiler_params=pltpu.CompilerParams(vmem_limit_bytes=8 * 1024 * 1024),
        cost_estimate=pl.CostEstimate(flops=flops, bytes_accessed=500_000, transcendentals=0),
    )(*args)


def local(fields, forcing, obs_cell, obs_count, obs_value, obs_var):
    members, rows, lon = fields.shape
    strips = lax.axis_size("lat")
    height = STEPS * members + 2 * STEPS
    fields, forcing = (pltpu.with_memory_space_constraint(value, pltpu.HBM) for value in (fields, forcing))
    top, bottom = call(
        pack_kernel,
        [(height, lon)] * 2,
        [HBM, HBM],
        (fields, forcing),
        [pltpu.VMEM(fields.shape, jnp.float32), pltpu.VMEM(forcing.shape, jnp.float32), pltpu.SemaphoreType.DMA((2,))],
    )
    up = [(i, i + 1) for i in range(strips - 1)]
    down = [(j, i) for i, j in up]
    before = lax.ppermute(bottom, "lat", up)
    after = lax.ppermute(top, "lat", down)
    early, kept, observed = call(
        functools.partial(early_kernel, strips - 1),
        [(NEAR, members, LANES), (6, members, lon), (8, LANES)],
        [VMEM] * 7,
        (obs_count, obs_cell, obs_value, obs_var, before, top, bottom),
        flops=10_000_000,
    )
    states = call(
        functools.partial(late_kernel, strips - 1),
        (NEAR, members, lon),
        [VMEM] * 4,
        (bottom, after, kept, early),
    )
    states = lax.all_to_all(states, "mem", 0, 0, axis_index_groups=NEAR_GROUPS, tiled=True)
    states = states.reshape(NEAR * members, lon)
    partial = call(moments_kernel, (CELLS + 8, LANES), [VMEM, VMEM], (states, observed))
    def exchange(value, *pairs):
        groups = [[first * NEAR + near, second * NEAR + near] for first, second in pairs for near in range(NEAR)]
        return lax.all_gather(value, "mem", axis_index_groups=groups)

    near_pair = exchange(partial, (0, 1), (2, 3))
    summed = near_pair[0, :CELLS] + near_pair[1, :CELLS]
    merged = jnp.concatenate([summed, near_pair[0, CELLS:], near_pair[1, CELLS:]], axis=0)
    received = exchange(merged, (0, 3), (1, 2))
    result = call(analyse_kernel, states.shape, [VMEM, VMEM], (received, states))
    result = result.reshape(NEAR, members, lon)
    result = lax.all_to_all(result, "mem", 0, 0, axis_index_groups=NEAR_GROUPS, tiled=True)
    return call(unpack_kernel, (members, rows, lon), [VMEM], (result,))


def solution(mesh):
    placed = (
        P("mem", "lat", None),
        P("lat", None),
        P("lat", None, None),
        P("lat", "mem"),
        P("lat", "mem", None),
        P("lat", "mem", None),
    )
    return jax.shard_map(local, mesh=mesh, in_specs=placed, out_specs=P("mem", "lat", None), check_vma=False)
```

```python
import functools

import jax
import jax.numpy as jnp
from jax import lax
from jax.experimental import pallas as pl
from jax.experimental.pallas import tpu as pltpu
from jax.sharding import PartitionSpec as P

CELLS = 64
STEPS = 4
TIME_STEP = 0.05
LAT_MIXING = 4.0
NEAR = 8
FAR = 4
HIGHEST = lax.Precision.HIGHEST
LANES = 128
NEAR_GROUPS = [[hi * NEAR + near for near in range(NEAR)] for hi in range(FAR)]


def low_half(shape):
    return lax.broadcasted_iota(jnp.int32, shape, 1) < CELLS


def halves(left, left_half, right, right_half):
    left = left if left_half == 0 else pltpu.roll(left, CELLS, 1)
    right = right if right_half == 1 else pltpu.roll(right, CELLS, 1)
    return jnp.where(low_half(left.shape), left, right)


def pack_kernel(fields, forcing, top, bottom, held, edges, sems):
    members = fields.shape[0]
    copies = [pltpu.make_async_copy(fields, held, sems.at[0]), pltpu.make_async_copy(forcing, edges, sems.at[1])]
    for copy in copies:
        copy.start()
    for copy in copies:
        copy.wait()
    for out, start in ((bottom, STEPS), (top, 0)):
        for row in range(STEPS):
            out[pl.ds(row * members, members), :] = held[:, start + row, :]
        edge = edges[pl.ds(start, STEPS), :]
        out[pl.ds(STEPS * members, 2 * STEPS), :] = jnp.concatenate([edge, edge], axis=0)


def observe(count, cells, values, variances, out):
    slots = values.shape[2]
    live = lax.broadcasted_iota(jnp.int32, (1, slots), 1) < count[...]
    weight = jnp.where(live, 1.0 / variances[0], 0.0)
    scaled = weight * values[0]
    mine = cells[0, pl.ds(lax.axis_index("mem"), 1), :]
    cell = lax.broadcasted_iota(jnp.int32, (2 * CELLS, slots), 0) % CELLS
    hit = jnp.where(cell == mine, 1.0, 0.0)
    row = lax.broadcasted_iota(jnp.int32, (8, slots), 0)
    terms = jnp.where(row == 0, weight, jnp.where(row == 1, scaled, 0.0))
    sums = lax.dot_general(
        terms, hit, (((1,), (1,)), ((), ())), precision=HIGHEST, preferred_element_type=jnp.float32
    )
    both = jnp.where(low_half((1, LANES)), sums[0:1], sums[1:2])
    out[...] = jnp.broadcast_to(both, (8, LANES))


def step_rows(rows, places, forces, strip, last_strip):
    updated = {}
    for place in places:
        here = rows[place]
        eastern = pltpu.roll(here, here.shape[1] - 1, 1)
        western = pltpu.roll(here, 1, 1)
        far_west = pltpu.roll(here, 2, 1)
        tendency = (
            (eastern - far_west) * western
            - here
            + forces(place)
            + LAT_MIXING * (rows[place - 1] + rows[place + 1] - 2.0 * here)
        )
        value = here + TIME_STEP * tendency
        if place < STEPS:
            value = jnp.where(strip == 0, 0.0, value)
        if place >= 3 * STEPS:
            value = jnp.where(strip == last_strip, 0.0, value)
        updated[place] = value
    return updated


def spread_patches(out, lanes_at, tile, rows):
    for near in range(NEAR):
        block = near % 4
        lanes = slice(block // 2 * LANES, block // 2 * LANES + LANES)
        first, second = rows[near // 4][:, lanes], rows[2 + near // 4][:, lanes]
        joined = halves(first, block % 2, second, block % 2)
        out[near, pl.ds(tile * first.shape[0], first.shape[0]), pl.ds(lanes_at, LANES)] = joined


def early_kernel(last_strip, count, cells, values, variances, before, top, bottom, out, kept, observed):
    observe(count, cells, values, variances, observed)
    members = out.shape[1]
    strip = lax.axis_index("lat")
    sources = [before, top, bottom]

    def forces(place):
        return sources[place // STEPS][pl.ds(STEPS * members + place % STEPS, 1), :]

    for tile in range(members // 32):
        rows = {
            place: sources[place // STEPS][pl.ds((place % STEPS) * members + tile * 32, 32), :]
            for place in range(3 * STEPS)
        }
        for step in range(STEPS):
            rows = step_rows(rows, range(1 + step, 11 - step), forces, strip, last_strip)
            if step < STEPS - 1:
                for place in range(2):
                    kept[2 * step + place, pl.ds(tile * 32, 32), :] = rows[9 - step + place]
        spread_patches(out, 0, tile, [rows[place] for place in range(4, 8)])


def late_kernel(last_strip, bottom, after, kept, early, out):
    members = out.shape[1]
    strip = lax.axis_index("lat")
    sources = [None, None, bottom, after]

    def forces(place):
        return sources[place // STEPS][pl.ds(STEPS * members + place % STEPS, 1), :]

    out[:, :, pl.ds(0, LANES)] = early[...]
    for tile in range(members // 32):
        rows = {
            place: sources[place // STEPS][pl.ds((place % STEPS) * members + tile * 32, 32), :]
            for place in range(10, 16)
        }
        for step in range(STEPS):
            if step > 0:
                for place in range(2):
                    rows[10 - step + place] = kept[2 * step - 2 + place, pl.ds(tile * 32, 32), :]
            rows = step_rows(rows, range(11 - step, 15 - step), forces, strip, last_strip)
        spread_patches(out, LANES, tile, [rows[place] for place in range(8, 12)])


def fold(square):
    return jnp.where(low_half((CELLS, LANES)), square[:CELLS], square[CELLS:])


def unfold(pair):
    low = low_half(pair.shape)
    return jnp.concatenate([jnp.where(low, pair, 0.0), jnp.where(low, 0.0, pair)], axis=0)


def places(shape):
    row = lax.broadcasted_iota(jnp.int32, shape, 0)
    return row, lax.broadcasted_iota(jnp.int32, shape, 1) % CELLS


def pack_symmetric(pair):
    side = CELLS // 2
    row, lane = places((side, LANES))
    take_upper = (lane >= side) & (row > lane - side)
    packed = jnp.where(take_upper, pltpu.roll(pair[:side], side, 1), pair[side:])
    return packed, jnp.sum(jnp.where(row == lane, pair[:side], 0.0), axis=0, keepdims=True)


def unpack_symmetric(packed, diagonals):
    side = CELLS // 2
    across = [halves(packed[0], half, packed[1], half) for half in range(2)]
    stacked = []
    for block in across:
        stacked += [pltpu.roll(block, LANES - side, 1), block]
    turned = jnp.concatenate(stacked, axis=0).T
    row, lane = places((CELLS, LANES))
    direct = ((lane < side) & (row > lane)) | ((lane >= side) & (row >= side) & (row <= lane))
    pairs = []
    for half in range(2):
        straight = jnp.concatenate([pltpu.roll(packed[half], LANES - side, 1), packed[half]], axis=0)
        full = jnp.where(direct, straight, turned[half * CELLS:(half + 1) * CELLS])
        pairs.append(jnp.where((row == lane) & (row < side), diagonals[half], full))
    return pairs


def moments_kernel(states, observed, out):
    mean = jnp.sum(states[...], axis=0, keepdims=True) / states.shape[0]
    centred = states[...] - mean
    square = lax.dot_general(
        centred, centred, (((0,), (0,)), ((), ())), precision=HIGHEST, preferred_element_type=jnp.float32
    )
    lines = []
    for half in range(2):
        lanes = slice(half * LANES, half * LANES + LANES)
        packed, diagonal = pack_symmetric(fold(square[lanes, lanes]))
        out[pl.ds(half * CELLS // 2, CELLS // 2), :] = packed
        lines += [mean[:, lanes], diagonal]
    row = lax.broadcasted_iota(jnp.int32, (8, LANES), 0)
    tail = observed[...]
    for place, line in enumerate(lines):
        tail = jnp.where(row == place, line, tail)
    out[pl.ds(CELLS, 8), :] = tail


def invert(pairs):
    row, lane = places((8, LANES))
    base = jnp.where(low_half((8, LANES)), 0, CELLS)

    def spread(block, line):
        return jnp.broadcast_to(block[line:line + 1, :], (8, LANES))

    for tile in range(8):
        inside = lane // 8 == tile
        identity = jnp.where(lane == row + 8 * tile, 1.0, 0.0)
        near = (tile, (tile + 1) % 8)
        columns = [
            [
                [
                    jnp.take_along_axis(part, base + (8 * tile + c), axis=1, mode="promise_in_bounds")
                    for c in range(8)
                ]
                if place in near
                else None
                for place, part in enumerate(pair)
            ]
            for pair in pairs
        ]
        inverses = [list(factors[tile]) for factors in columns]
        for line in range(8):
            for inverse in inverses:
                reciprocal = 1.0 / spread(inverse[line], line)
                for c in range(8):
                    if c != line:
                        lead = spread(inverse[c], line) * reciprocal
                        inverse[c] = jnp.where(row == line, lead, inverse[c] - inverse[line] * lead)
                inverse[line] = jnp.where(row == line, reciprocal, -inverse[line] * reciprocal)
        for pair, factors, inverse in zip(pairs, columns, inverses):
            block = jnp.where(inside, identity, pair[tile])
            lead = inverse[0] * spread(block, 0)
            for c in range(1, 8):
                lead = lead + inverse[c] * spread(block, c)
            whole = jnp.concatenate(pair, axis=0)
            across = jnp.where(places((CELLS, LANES))[1] // 8 == tile, whole, 0.0)
            low = low_half((8, LANES))
            empty = jnp.zeros((8, LANES), jnp.float32)
            rows = [empty] * 16
            rows[tile] = jnp.where(low, lead, 0.0)
            rows[8 + tile] = jnp.where(low, 0.0, lead)
            product = jnp.dot(
                across, jnp.concatenate(rows, axis=0), precision=HIGHEST, preferred_element_type=jnp.float32
            )
            for place in range(8):
                if place not in near:
                    pair[place] = jnp.where(inside, 0.0, pair[place]) - product[8 * place:8 * place + 8]
            pair[tile] = lead
            leads = [spread(lead, c) for c in range(8)]
            for place in near:
                if place != tile:
                    rest = jnp.where(inside, 0.0, pair[place])
                    for c in range(8):
                        rest = rest - factors[place][c] * leads[c]
                    pair[place] = rest


def analyse_kernel(received, states, out):
    group = states.shape[0]
    members = FAR * group
    side = CELLS // 2

    def line(hi, place):
        return received[hi // 2, pl.ds(CELLS + 8 * (hi % 2) + place, 1), :]

    def observed(hi):
        return line(hi, 4)

    def total(part):
        return part(0) + part(1) + part(2) + part(3)

    packed = [received[0, pl.ds(half * side, side), :] + received[1, pl.ds(half * side, side), :] for half in range(2)]
    within = unpack_symmetric(packed, [total(lambda hi: line(hi, 2 * half + 1)) for half in range(2)])
    row, lane = places((CELLS, LANES))
    identity = jnp.where(row == lane, 1.0, 0.0)
    means, weights, shifts, pairs = [], [], [], []
    for half in range(2):
        mean = total(lambda hi: line(hi, 2 * half)) / FAR
        which = lax.broadcasted_iota(jnp.int32, (8, LANES), 0)
        offsets = jnp.zeros((8, LANES), jnp.float32)
        for hi in range(FAR):
            offsets = jnp.where(which == hi, line(hi, 2 * half) - mean, offsets)
        between = lax.dot_general(
            offsets, offsets, (((0,), (0,)), ((), ())), precision=HIGHEST, preferred_element_type=jnp.float32
        )
        covariance = (within[half] + group * fold(between)) / (members - 1)
        first, second = observed(2 * half), observed(2 * half + 1)
        weight = halves(first, 0, second, 0)
        shift = halves(first, 1, second, 1) - weight * mean
        shift = jnp.dot(
            jnp.broadcast_to(shift, (8, LANES)),
            unfold(covariance),
            precision=HIGHEST,
            preferred_element_type=jnp.float32,
        )
        system = covariance * weight + identity
        means.append(mean)
        shifts.append(shift[:1])
        pairs.append([system[8 * tile:8 * tile + 8] for tile in range(8)])
    invert(pairs)
    block = states[...]
    spread = 0.5 * (block - jnp.concatenate(means, axis=1))
    gains = [unfold(jnp.concatenate(pair, axis=0)) for pair in pairs]
    empty = jnp.zeros((LANES, LANES), jnp.float32)
    gain = jnp.concatenate(
        [jnp.concatenate([gains[0], empty], axis=1), jnp.concatenate([empty, gains[1]], axis=1)], axis=0
    )
    out[...] = (block - spread) + lax.dot_general(
        spread + jnp.concatenate(shifts, axis=1),
        gain,
        (((1,), (1,)), ((), ())),
        precision=HIGHEST,
        preferred_element_type=jnp.float32,
    )


def unpack_kernel(arrived, out):
    for row in range(out.shape[1]):
        hi, side = divmod(row, 2)
        lanes = pl.ds(hi // 2 * LANES, LANES)
        for pair in range(2):
            near = 4 * side + 2 * pair
            joined = halves(arrived[near, :, lanes], hi % 2, arrived[near + 1, :, lanes], hi % 2)
            out[:, row, pl.ds(pair * LANES, LANES)] = joined


VMEM = pl.BlockSpec(memory_space=pltpu.VMEM)
HBM = pl.BlockSpec(memory_space=pltpu.HBM)


def call(kernel, outs, in_specs, args, scratch=(), flops=1_000_000):
    many = isinstance(outs, list)
    shapes = [jax.ShapeDtypeStruct(s, jnp.float32) for s in (outs if many else [outs])]
    return pl.pallas_call(
        kernel,
        out_shape=shapes if many else shapes[0],
        in_specs=in_specs,
        out_specs=[VMEM] * len(shapes) if many else VMEM,
        scratch_shapes=list(scratch),
        compiler_params=pltpu.CompilerParams(vmem_limit_bytes=8 * 1024 * 1024),
        cost_estimate=pl.CostEstimate(flops=flops, bytes_accessed=500_000, transcendentals=0),
    )(*args)


def local(fields, forcing, obs_cell, obs_count, obs_value, obs_var):
    members, rows, lon = fields.shape
    strips = lax.axis_size("lat")
    height = STEPS * members + 2 * STEPS
    fields, forcing = (pltpu.with_memory_space_constraint(value, pltpu.HBM) for value in (fields, forcing))
    top, bottom = call(
        pack_kernel,
        [(height, lon)] * 2,
        [HBM, HBM],
        (fields, forcing),
        [pltpu.VMEM(fields.shape, jnp.float32), pltpu.VMEM(forcing.shape, jnp.float32), pltpu.SemaphoreType.DMA((2,))],
    )
    up = [(i, i + 1) for i in range(strips - 1)]
    down = [(j, i) for i, j in up]
    before = lax.ppermute(bottom, "lat", up)
    after = lax.ppermute(top, "lat", down)
    early, kept, observed = call(
        functools.partial(early_kernel, strips - 1),
        [(NEAR, members, LANES), (6, members, lon), (8, LANES)],
        [VMEM] * 7,
        (obs_count, obs_cell, obs_value, obs_var, before, top, bottom),
        flops=10_000_000,
    )
    states = call(
        functools.partial(late_kernel, strips - 1),
        (NEAR, members, lon),
        [VMEM] * 4,
        (bottom, after, kept, early),
    )
    states = lax.all_to_all(states, "mem", 0, 0, axis_index_groups=NEAR_GROUPS, tiled=True)
    states = states.reshape(NEAR * members, lon)
    partial = call(moments_kernel, (CELLS + 8, LANES), [VMEM, VMEM], (states, observed))
    def exchange(value, *pairs):
        groups = [[first * NEAR + near, second * NEAR + near] for first, second in pairs for near in range(NEAR)]
        return lax.all_gather(value, "mem", axis_index_groups=groups)

    near_pair = exchange(partial, (0, 1), (2, 3))
    summed = near_pair[0, :CELLS] + near_pair[1, :CELLS]
    merged = jnp.concatenate([summed, near_pair[0, CELLS:], near_pair[1, CELLS:]], axis=0)
    received = exchange(merged, (0, 3), (1, 2))
    result = call(analyse_kernel, states.shape, [VMEM, VMEM], (received, states))
    result = result.reshape(NEAR, members, lon)
    result = lax.all_to_all(result, "mem", 0, 0, axis_index_groups=NEAR_GROUPS, tiled=True)
    return call(unpack_kernel, (members, rows, lon), [VMEM], (result,))


def solution(mesh):
    placed = (
        P("mem", "lat", None),
        P("lat", None),
        P("lat", None, None),
        P("lat", "mem"),
        P("lat", "mem", None),
        P("lat", "mem", None),
    )
    return jax.shard_map(local, mesh=mesh, in_specs=placed, out_specs=P("mem", "lat", None), check_vma=False)
```

```python
import functools

import jax
import jax.numpy as jnp
from jax import lax
from jax.experimental import pallas as pl
from jax.experimental.pallas import tpu as pltpu
from jax.sharding import PartitionSpec as P

CELLS = 64
STEPS = 4
TIME_STEP = 0.05
LAT_MIXING = 4.0
NEAR = 8
FAR = 4
HIGHEST = lax.Precision.HIGHEST
LANES = 128
NEAR_GROUPS = [[hi * NEAR + near for near in range(NEAR)] for hi in range(FAR)]


def low_half(shape):
    return lax.broadcasted_iota(jnp.int32, shape, 1) < CELLS


def halves(left, left_half, right, right_half):
    left = left if left_half == 0 else pltpu.roll(left, CELLS, 1)
    right = right if right_half == 1 else pltpu.roll(right, CELLS, 1)
    return jnp.where(low_half(left.shape), left, right)


def pack_kernel(fields, forcing, top, bottom, held, edges, sems):
    members = fields.shape[0]
    copies = [pltpu.make_async_copy(fields, held, sems.at[0]), pltpu.make_async_copy(forcing, edges, sems.at[1])]
    for copy in copies:
        copy.start()
    for copy in copies:
        copy.wait()
    for out, start in ((bottom, STEPS), (top, 0)):
        for row in range(STEPS):
            out[pl.ds(row * members, members), :] = held[:, start + row, :]
        edge = edges[pl.ds(start, STEPS), :]
        out[pl.ds(STEPS * members, 2 * STEPS), :] = jnp.concatenate([edge, edge], axis=0)


def observe(count, cells, values, variances, out):
    slots = values.shape[2]
    live = lax.broadcasted_iota(jnp.int32, (1, slots), 1) < count[...]
    weight = jnp.where(live, 1.0 / variances[0], 0.0)
    scaled = weight * values[0]
    mine = cells[0, pl.ds(lax.axis_index("mem"), 1), :]
    cell = lax.broadcasted_iota(jnp.int32, (2 * CELLS, slots), 0) % CELLS
    hit = jnp.where(cell == mine, 1.0, 0.0)
    row = lax.broadcasted_iota(jnp.int32, (8, slots), 0)
    terms = jnp.where(row == 0, weight, jnp.where(row == 1, scaled, 0.0))
    sums = lax.dot_general(
        terms, hit, (((1,), (1,)), ((), ())), precision=HIGHEST, preferred_element_type=jnp.float32
    )
    both = jnp.where(low_half((1, LANES)), sums[0:1], sums[1:2])
    out[...] = jnp.broadcast_to(both, (8, LANES))


def step_rows(rows, places, forces, strip, last_strip):
    updated = {}
    for place in places:
        here = rows[place]
        eastern = pltpu.roll(here, here.shape[1] - 1, 1)
        western = pltpu.roll(here, 1, 1)
        far_west = pltpu.roll(here, 2, 1)
        tendency = (
            (eastern - far_west) * western
            - here
            + forces(place)
            + LAT_MIXING * (rows[place - 1] + rows[place + 1] - 2.0 * here)
        )
        value = here + TIME_STEP * tendency
        if place < STEPS:
            value = jnp.where(strip == 0, 0.0, value)
        if place >= 3 * STEPS:
            value = jnp.where(strip == last_strip, 0.0, value)
        updated[place] = value
    return updated


def spread_patches(out, lanes_at, tile, rows):
    for near in range(NEAR):
        block = near % 4
        lanes = slice(block // 2 * LANES, block // 2 * LANES + LANES)
        first, second = rows[near // 4][:, lanes], rows[2 + near // 4][:, lanes]
        joined = halves(first, block % 2, second, block % 2)
        out[near, pl.ds(tile * first.shape[0], first.shape[0]), pl.ds(lanes_at, LANES)] = joined


def early_kernel(last_strip, count, cells, values, variances, before, top, bottom, out, kept, observed):
    observe(count, cells, values, variances, observed)
    members = out.shape[1]
    strip = lax.axis_index("lat")
    sources = [before, top, bottom]

    def forces(place):
        return sources[place // STEPS][pl.ds(STEPS * members + place % STEPS, 1), :]

    for tile in range(members // 32):
        rows = {
            place: sources[place // STEPS][pl.ds((place % STEPS) * members + tile * 32, 32), :]
            for place in range(3 * STEPS)
        }
        for step in range(STEPS):
            rows = step_rows(rows, range(1 + step, 11 - step), forces, strip, last_strip)
            if step < STEPS - 1:
                for place in range(2):
                    kept[2 * step + place, pl.ds(tile * 32, 32), :] = rows[9 - step + place]
        spread_patches(out, 0, tile, [rows[place] for place in range(4, 8)])


def late_kernel(last_strip, bottom, after, kept, early, out):
    members = out.shape[1]
    strip = lax.axis_index("lat")
    sources = [None, None, bottom, after]

    def forces(place):
        return sources[place // STEPS][pl.ds(STEPS * members + place % STEPS, 1), :]

    out[:, :, pl.ds(0, LANES)] = early[...]
    for tile in range(members // 32):
        rows = {
            place: sources[place // STEPS][pl.ds((place % STEPS) * members + tile * 32, 32), :]
            for place in range(10, 16)
        }
        for step in range(STEPS):
            if step > 0:
                for place in range(2):
                    rows[10 - step + place] = kept[2 * step - 2 + place, pl.ds(tile * 32, 32), :]
            rows = step_rows(rows, range(11 - step, 15 - step), forces, strip, last_strip)
        spread_patches(out, LANES, tile, [rows[place] for place in range(8, 12)])


def fold(square):
    return jnp.where(low_half((CELLS, LANES)), square[:CELLS], square[CELLS:])


def unfold(pair):
    low = low_half(pair.shape)
    return jnp.concatenate([jnp.where(low, pair, 0.0), jnp.where(low, 0.0, pair)], axis=0)


def places(shape):
    row = lax.broadcasted_iota(jnp.int32, shape, 0)
    return row, lax.broadcasted_iota(jnp.int32, shape, 1) % CELLS


def pack_symmetric(pair):
    side = CELLS // 2
    row, lane = places((side, LANES))
    take_upper = (lane >= side) & (row > lane - side)
    packed = jnp.where(take_upper, pltpu.roll(pair[:side], side, 1), pair[side:])
    return packed, jnp.sum(jnp.where(row == lane, pair[:side], 0.0), axis=0, keepdims=True)


def unpack_symmetric(packed, diagonals):
    side = CELLS // 2
    across = [halves(packed[0], half, packed[1], half) for half in range(2)]
    stacked = []
    for block in across:
        stacked += [pltpu.roll(block, LANES - side, 1), block]
    turned = jnp.concatenate(stacked, axis=0).T
    row, lane = places((CELLS, LANES))
    direct = ((lane < side) & (row > lane)) | ((lane >= side) & (row >= side) & (row <= lane))
    pairs = []
    for half in range(2):
        straight = jnp.concatenate([pltpu.roll(packed[half], LANES - side, 1), packed[half]], axis=0)
        full = jnp.where(direct, straight, turned[half * CELLS:(half + 1) * CELLS])
        pairs.append(jnp.where((row == lane) & (row < side), diagonals[half], full))
    return pairs


def moments_kernel(states, observed, out):
    mean = jnp.sum(states[...], axis=0, keepdims=True) / states.shape[0]
    centred = states[...] - mean
    square = lax.dot_general(
        centred, centred, (((0,), (0,)), ((), ())), precision=HIGHEST, preferred_element_type=jnp.float32
    )
    lines = []
    for half in range(2):
        lanes = slice(half * LANES, half * LANES + LANES)
        packed, diagonal = pack_symmetric(fold(square[lanes, lanes]))
        out[pl.ds(half * CELLS // 2, CELLS // 2), :] = packed
        lines += [mean[:, lanes], diagonal]
    row = lax.broadcasted_iota(jnp.int32, (8, LANES), 0)
    tail = observed[...]
    for place, line in enumerate(lines):
        tail = jnp.where(row == place, line, tail)
    out[pl.ds(CELLS, 8), :] = tail


def invert(pairs):
    row, lane = places((8, LANES))
    base = jnp.where(low_half((8, LANES)), 0, CELLS)

    def spread(block, line):
        return jnp.broadcast_to(block[line:line + 1, :], (8, LANES))

    for tile in range(8):
        inside = lane // 8 == tile
        identity = jnp.where(lane == row + 8 * tile, 1.0, 0.0)
        near = (tile, (tile + 1) % 8)
        columns = [
            [
                [
                    jnp.take_along_axis(part, base + (8 * tile + c), axis=1, mode="promise_in_bounds")
                    for c in range(8)
                ]
                if place in near
                else None
                for place, part in enumerate(pair)
            ]
            for pair in pairs
        ]
        inverses = [list(factors[tile]) for factors in columns]
        for line in range(8):
            for inverse in inverses:
                reciprocal = 1.0 / spread(inverse[line], line)
                for c in range(8):
                    if c != line:
                        lead = spread(inverse[c], line) * reciprocal
                        inverse[c] = jnp.where(row == line, lead, inverse[c] - inverse[line] * lead)
                inverse[line] = jnp.where(row == line, reciprocal, -inverse[line] * reciprocal)
        for pair, factors, inverse in zip(pairs, columns, inverses):
            block = jnp.where(inside, identity, pair[tile])
            lead = inverse[0] * spread(block, 0)
            for c in range(1, 8):
                lead = lead + inverse[c] * spread(block, c)
            whole = jnp.concatenate(pair, axis=0)
            across = jnp.where(places((CELLS, LANES))[1] // 8 == tile, whole, 0.0)
            low = low_half((8, LANES))
            empty = jnp.zeros((8, LANES), jnp.float32)
            rows = [empty] * 16
            rows[tile] = jnp.where(low, lead, 0.0)
            rows[8 + tile] = jnp.where(low, 0.0, lead)
            product = jnp.dot(
                across, jnp.concatenate(rows, axis=0), precision=HIGHEST, preferred_element_type=jnp.float32
            )
            for place in range(8):
                if place not in near:
                    pair[place] = jnp.where(inside, 0.0, pair[place]) - product[8 * place:8 * place + 8]
            pair[tile] = lead
            leads = [spread(lead, c) for c in range(8)]
            for place in near:
                if place != tile:
                    rest = jnp.where(inside, 0.0, pair[place])
                    for c in range(8):
                        rest = rest - factors[place][c] * leads[c]
                    pair[place] = rest


def analyse_kernel(received, states, out):
    group = states.shape[0]
    members = FAR * group
    side = CELLS // 2

    def line(hi, place):
        return received[hi // 2, pl.ds(CELLS + 8 * (hi % 2) + place, 1), :]

    def observed(hi):
        return line(hi, 4)

    def total(part):
        return part(0) + part(1) + part(2) + part(3)

    packed = [received[0, pl.ds(half * side, side), :] + received[1, pl.ds(half * side, side), :] for half in range(2)]
    within = unpack_symmetric(packed, [total(lambda hi: line(hi, 2 * half + 1)) for half in range(2)])
    row, lane = places((CELLS, LANES))
    identity = jnp.where(row == lane, 1.0, 0.0)
    means, weights, shifts, pairs = [], [], [], []
    for half in range(2):
        mean = total(lambda hi: line(hi, 2 * half)) / FAR
        which = lax.broadcasted_iota(jnp.int32, (8, LANES), 0)
        offsets = jnp.zeros((8, LANES), jnp.float32)
        for hi in range(FAR):
            offsets = jnp.where(which == hi, line(hi, 2 * half) - mean, offsets)
        between = lax.dot_general(
            offsets, offsets, (((0,), (0,)), ((), ())), precision=HIGHEST, preferred_element_type=jnp.float32
        )
        covariance = (within[half] + group * fold(between)) / (members - 1)
        first, second = observed(2 * half), observed(2 * half + 1)
        weight = halves(first, 0, second, 0)
        seen = weight > 0.0
        target = halves(first, 1, second, 1) / jnp.where(seen, weight, 1.0)
        shifts.append(jnp.where(seen, target - mean, 0.0))
        system = covariance * weight + identity
        means.append(mean)
        pairs.append([system[8 * tile:8 * tile + 8] for tile in range(8)])
    invert(pairs)
    block = states[...]
    spread = 0.5 * (block - jnp.concatenate(means, axis=1))
    gains = [unfold(jnp.concatenate(pair, axis=0)) for pair in pairs]
    empty = jnp.zeros((LANES, LANES), jnp.float32)
    gain = jnp.concatenate(
        [jnp.concatenate([gains[0], empty], axis=1), jnp.concatenate([empty, gains[1]], axis=1)], axis=0
    )
    shift = jnp.concatenate(shifts, axis=1)
    out[...] = (block - spread) + shift + lax.dot_general(
        spread - shift,
        gain,
        (((1,), (1,)), ((), ())),
        precision=HIGHEST,
        preferred_element_type=jnp.float32,
    )


def unpack_kernel(arrived, out):
    for row in range(out.shape[1]):
        hi, side = divmod(row, 2)
        lanes = pl.ds(hi // 2 * LANES, LANES)
        for pair in range(2):
            near = 4 * side + 2 * pair
            joined = halves(arrived[near, :, lanes], hi % 2, arrived[near + 1, :, lanes], hi % 2)
            out[:, row, pl.ds(pair * LANES, LANES)] = joined


VMEM = pl.BlockSpec(memory_space=pltpu.VMEM)
HBM = pl.BlockSpec(memory_space=pltpu.HBM)


def call(kernel, outs, in_specs, args, scratch=(), flops=1_000_000):
    many = isinstance(outs, list)
    shapes = [jax.ShapeDtypeStruct(s, jnp.float32) for s in (outs if many else [outs])]
    return pl.pallas_call(
        kernel,
        out_shape=shapes if many else shapes[0],
        in_specs=in_specs,
        out_specs=[VMEM] * len(shapes) if many else VMEM,
        scratch_shapes=list(scratch),
        compiler_params=pltpu.CompilerParams(vmem_limit_bytes=8 * 1024 * 1024),
        cost_estimate=pl.CostEstimate(flops=flops, bytes_accessed=500_000, transcendentals=0),
    )(*args)


def local(fields, forcing, obs_cell, obs_count, obs_value, obs_var):
    members, rows, lon = fields.shape
    strips = lax.axis_size("lat")
    height = STEPS * members + 2 * STEPS
    fields, forcing = (pltpu.with_memory_space_constraint(value, pltpu.HBM) for value in (fields, forcing))
    top, bottom = call(
        pack_kernel,
        [(height, lon)] * 2,
        [HBM, HBM],
        (fields, forcing),
        [pltpu.VMEM(fields.shape, jnp.float32), pltpu.VMEM(forcing.shape, jnp.float32), pltpu.SemaphoreType.DMA((2,))],
    )
    up = [(i, i + 1) for i in range(strips - 1)]
    down = [(j, i) for i, j in up]
    before = lax.ppermute(bottom, "lat", up)
    after = lax.ppermute(top, "lat", down)
    early, kept, observed = call(
        functools.partial(early_kernel, strips - 1),
        [(NEAR, members, LANES), (6, members, lon), (8, LANES)],
        [VMEM] * 7,
        (obs_count, obs_cell, obs_value, obs_var, before, top, bottom),
        flops=10_000_000,
    )
    states = call(
        functools.partial(late_kernel, strips - 1),
        (NEAR, members, lon),
        [VMEM] * 4,
        (bottom, after, kept, early),
    )
    states = lax.all_to_all(states, "mem", 0, 0, axis_index_groups=NEAR_GROUPS, tiled=True)
    states = states.reshape(NEAR * members, lon)
    partial = call(moments_kernel, (CELLS + 8, LANES), [VMEM, VMEM], (states, observed))
    def exchange(value, *pairs):
        groups = [[first * NEAR + near, second * NEAR + near] for first, second in pairs for near in range(NEAR)]
        return lax.all_gather(value, "mem", axis_index_groups=groups)

    near_pair = exchange(partial, (0, 1), (2, 3))
    summed = near_pair[0, :CELLS] + near_pair[1, :CELLS]
    merged = jnp.concatenate([summed, near_pair[0, CELLS:], near_pair[1, CELLS:]], axis=0)
    received = exchange(merged, (0, 3), (1, 2))
    result = call(analyse_kernel, states.shape, [VMEM, VMEM], (received, states))
    result = result.reshape(NEAR, members, lon)
    result = lax.all_to_all(result, "mem", 0, 0, axis_index_groups=NEAR_GROUPS, tiled=True)
    return call(unpack_kernel, (members, rows, lon), [VMEM], (result,))


def solution(mesh):
    placed = (
        P("mem", "lat", None),
        P("lat", None),
        P("lat", None, None),
        P("lat", "mem"),
        P("lat", "mem", None),
        P("lat", "mem", None),
    )
    return jax.shard_map(local, mesh=mesh, in_specs=placed, out_specs=P("mem", "lat", None), check_vma=False)
```
